128 devices in a mesh: row: 16 (over x, y), col: 8 (over z, core).
Axes of the slice: x: 4, y: 4, z: 4, core: 2. Of those that a mesh axis runs over, the one named last changes fastest.
Arguments:
- surface: bfloat16 [16384, 16384], P('row', 'col'), may hold values from -0.0234375 to 0.0234375
- excitation: float32 [16384, 128], P(('row', 'col')), may hold values from -6 to 6
- dtn_blocks: bfloat16 [128, 1024, 1024], P(('row', 'col')), may hold values from -0.09375 to 0.09375
- interp_blocks: bfloat16 [128, 1024, 1024], P(('row', 'col')), may hold values from -0.125 to 0.125
- adjacency: int32 [128, 6], P(('row', 'col')), may hold values from 0 to 127, as said below
Outputs:
- solution: float32 [16384, 128], P(('row', 'col'))
- residual: float32 [16384, 128], P(('row', 'col'))
The draws below stay inside these ranges and needn't reach their ends.
Inputs may be any that keep to these rules, and one draw needn't show every extreme that they name: `adjacency`: entry [s, k] names a subdomain of the same spatial group as s (equal index // 8); it may name s itself, which adds nothing.
All inputs are finite; a program needn't handle non-finite values.
Results may differ from the reference program's by a relative error of at most 0.02.
Values may be sent and summed in bfloat16 or wider, within the bound.
No kernel may reach another device: no remote copies, remote signals or barrier semaphores. Data moves between devices by JAX's collectives and lax.ppermute only.
A program may use at most 64 MiB of HBM per device.

```python
import jax
import jax.numpy as jnp
from jax import lax

NS = 16384
M = 1024
NE = 128
ITERS = 2
NADJ = 6
NSUB = 128
GROUP = 8
RB = 1024
N_ROW = 16


def draw_adjacency(key, part):
    base = jnp.arange(NSUB, dtype=jnp.int32) // GROUP * GROUP
    offsets = jax.random.randint(jax.random.fold_in(key, 17), (NSUB, NADJ), 0, GROUP, dtype=jnp.int32)
    return base[:, None] + offsets


def block_scale(stream_key, shape, cuts, smallest, top_value):
    factor_of = 1.0
    for axis_at, shards_of in cuts:
        steps = jax.random.uniform(jax.random.fold_in(jax.random.fold_in(stream_key, 6), axis_at), (shards_of,), jnp.float32, smallest / len(cuts), top_value / len(cuts))
        factor_of = factor_of * jnp.repeat(jnp.exp(steps), shape[axis_at] // shards_of).reshape((-1,) + (1,) * (len(shape) - 1 - axis_at))
    return factor_of


def gaussian(stream_key, shape, deviation, reach, shards=(), held_as=jnp.bfloat16):
    result = deviation * jax.random.normal(stream_key, shape, jnp.float32)
    if shards:
        result = result * block_scale(stream_key, shape, shards, -0.22, 0.18)
    return jnp.clip(result, -reach, reach).astype(held_as)


def setup_inputs(seed: int = 0) -> dict:
    seeds = jax.random.split(jax.random.key(seed), 6)
    return {
        "surface": gaussian(seeds[0], (NS, NS), (4 * NS) ** -0.5, 0.0234375, ((0, 16), (1, 8))),
        "excitation": gaussian(seeds[1], (NS, NE), 1.0, 6.0, ((0, 128),), jnp.float32),
        "dtn_blocks": gaussian(seeds[2], (NSUB, M, M), (4 * M) ** -0.5, 0.09375, ((0, 128),)),
        "interp_blocks": gaussian(seeds[3], (NSUB, M, RB), (2 * RB) ** -0.5, 0.125, ((0, 128),)),
        "adjacency": draw_adjacency(jax.random.fold_in(seeds[5], 71), 0),
    }


damping = 0.25
face_weight = 0.25


def reference(surface, excitation, dtn_blocks, interp_blocks, adjacency):
    current = excitation
    residual = excitation
    indices = jnp.arange(NSUB, dtype=jnp.int32)
    for sweep in range(ITERS):
        rounded = current.astype(jnp.bfloat16)
        applied = jnp.dot(surface, rounded, preferred_element_type=jnp.float32)
        grouped = rounded.reshape(N_ROW, RB, NE)

        def trace_one(index):
            block = lax.dynamic_index_in_dim(grouped, index // GROUP, 0, keepdims=False)
            return jnp.dot(interp_blocks[index], block, preferred_element_type=jnp.float32).astype(jnp.bfloat16)

        traces = lax.map(trace_one, indices)

        def respond(index):
            own = traces[index]
            own_wide = own.astype(jnp.float32)
            neighbours = jnp.zeros((M, NE), jnp.float32)
            for slot in range(NADJ):
                neighbours = neighbours + traces[adjacency[index, slot]].astype(jnp.float32)
            combined = jnp.dot(dtn_blocks[index], own, preferred_element_type=jnp.float32) + own_wide
            combined = combined + face_weight * (NADJ * own_wide - neighbours)
            response = combined.astype(jnp.bfloat16)
            return lax.dot_general(interp_blocks[index], response, (((0,), (0,)), ((), ())), preferred_element_type=jnp.float32)

        returned = lax.map(respond, indices)
        back = returned.reshape(N_ROW, GROUP, RB, NE).sum(axis=1).reshape(NS, NE)
        residual = excitation - current - applied - back
        current = current + damping * residual
    return current, residual
```

```python
import jax
import jax.numpy as jnp
from jax import lax
from jax.sharding import PartitionSpec as P

ITERS = 2
NADJ = 6

damping = 0.25
face_weight = 0.25

BF = jnp.bfloat16
F32 = jnp.float32


def dot(a, b):
    return jnp.dot(a, b, preferred_element_type=F32)


def dot_t(a, b):
    return lax.dot_general(a, b, (((0,), (0,)), ((), ())), preferred_element_type=F32)


def exchange(blocks, axis):
    return lax.all_to_all(blocks, axis, split_axis=0, concat_axis=0, tiled=True)


def copy_for_each(shard, axis):
    return exchange(jnp.broadcast_to(shard, (lax.axis_size(axis), *shard.shape)), axis)


def turned(rows, cols):
    per_col = rows // cols
    return [
        (r * cols + c, ((r % per_col) * cols + c) * cols + r // per_col)
        for r in range(rows)
        for c in range(cols)
    ]


def local(surface, excitation, dtn_blocks, interp_blocks, adjacency):
    cols = lax.axis_size("col")
    rows = lax.axis_size("row")
    dtn = dtn_blocks[0]
    interp = interp_blocks[0]
    m, rb = interp.shape
    ms = m // cols
    n, ne = excitation.shape

    with jax.named_scope("slices"):
        slices = exchange(interp.reshape(cols, ms, rb), "col")

    adjacent = adjacency[0] % cols
    owners = jnp.arange(ne, dtype=jnp.int32)
    counts = jnp.sum((adjacent[None, :] == owners[:, None]).astype(F32), axis=1)
    me = (owners == lax.axis_index("col")).astype(F32)
    weights = (1.0 + face_weight * NADJ) * me - face_weight * counts
    extra = jnp.broadcast_to(weights.astype(BF)[None, :], (16, ne))

    own = dot_t(interp, dot(dtn, interp).astype(BF))
    current = excitation
    residual = excitation
    operator = None
    for sweep in range(ITERS):
        rounded = current.astype(BF)
        with jax.named_scope("turn"):
            piece = lax.ppermute(rounded, ("row", "col"), turned(rows, cols))
        with jax.named_scope("columns"):
            column_block = copy_for_each(piece, "row").reshape(rows * n, ne)
        with jax.named_scope("group"):
            if sweep == 0:
                got = copy_for_each(jnp.concatenate([rounded, extra], axis=0), "col")
                group_block = got[:, :n].reshape(cols * n, ne)
                mix = got[:, n, :cols]
            else:
                group_block = copy_for_each(rounded, "col").reshape(cols * n, ne)
        if sweep == 0:
            tall = slices.reshape(m, rb)
            kind = jnp.repeat(jnp.repeat(mix, ms, axis=0), ms, axis=1)
            place = jnp.arange(m, dtype=jnp.int32) % ms
            spread = jnp.where(place[:, None] == place[None, :], kind, jnp.zeros((), BF))
            faces = dot_t(tall, dot(spread, tall).astype(BF))
            operator = (own + faces).astype(BF)
        part = dot(operator, group_block) + dot(surface, column_block)
        with jax.named_scope("result"):
            blocks = exchange(part.astype(BF).reshape(cols, n, ne), "col")
        summed = jnp.sum(blocks.astype(F32), axis=0)
        residual = excitation - current - summed
        current = current + damping * residual
    return (current, residual)


def solution(mesh):
    in_specs = (
        P("row", "col"),
        P(("row", "col"), None),
        P(("row", "col"), None, None),
        P(("row", "col"), None, None),
        P(("row", "col"), None),
    )
    out_specs = (P(("row", "col"), None), P(("row", "col"), None))
    return jax.shard_map(local, mesh=mesh, in_specs=in_specs, out_specs=out_specs, check_vma=False)
```

```python
import jax
import jax.numpy as jnp
from jax import lax
from jax.experimental import pallas as pl
from jax.experimental.pallas import tpu as pltpu
from jax.sharding import PartitionSpec as P


ITERS = 2
NADJ = 6

damping = 0.25
face_weight = 0.25

BF = jnp.bfloat16
F32 = jnp.float32


def dot(a, b):
    return jnp.dot(a, b, preferred_element_type=F32)


def dot_t(a, b):
    return lax.dot_general(a, b, (((0,), (0,)), ((), ())), preferred_element_type=F32)


def exchange(blocks, axis):
    return lax.all_to_all(blocks, axis, split_axis=0, concat_axis=0, tiled=True)


def copy_for_each(shard, axis):
    return exchange(jnp.broadcast_to(shard, (lax.axis_size(axis), *shard.shape)), axis)


def turned(rows, cols):
    per_col = rows // cols
    return [
        (r * cols + c, ((r % per_col) * cols + c) * cols + r // per_col)
        for r in range(rows)
        for c in range(cols)
    ]


def volume_kernel(interp_ref, dtn_ref, group_ref, out_ref):
    traces = dot(interp_ref[...], group_ref[...]).astype(BF)
    response = dot(dtn_ref[...], traces).astype(BF)
    out_ref[...] = dot_t(interp_ref[...], response)


def faces_kernel(*refs):
    mix_ref, prior_ref, group_ref = refs[:3]
    slice_refs = refs[3:-1]
    out_ref = refs[-1]
    peers = len(slice_refs)
    group = group_ref[...]
    traces = [dot(ref[...], group).astype(BF).astype(F32) for ref in slice_refs]
    total = prior_ref[...]
    for s in range(peers):
        mixed = mix_ref[s, 0] * traces[0]
        for p in range(1, peers):
            mixed = mixed + mix_ref[s, p] * traces[p]
        total = total + dot_t(slice_refs[s][...], mixed.astype(BF))
    out_ref[...] = total.astype(out_ref.dtype)


def surface_kernel(prior_ref, surface_ref, column_ref, out_ref):
    out_ref[...] = (prior_ref[...] + dot(surface_ref[...], column_ref[...])).astype(out_ref.dtype)


def vmem():
    return pl.BlockSpec(memory_space=pltpu.VMEM)


def volume(interp, dtn, group_block):
    shape = jax.ShapeDtypeStruct(group_block.shape, F32)
    return pl.pallas_call(
        volume_kernel, out_shape=shape, in_specs=[vmem()] * 3, out_specs=vmem(), name="volume"
    )(interp, dtn, group_block)


def applied(prior, surface, column_block, dtype):
    shape = jax.ShapeDtypeStruct(prior.shape, dtype)
    return pl.pallas_call(
        surface_kernel, out_shape=shape, in_specs=[vmem()] * 3, out_specs=vmem(), name="applied"
    )(prior, surface, column_block)


def faces(mix, prior, group_block, slices, dtype):
    shape = jax.ShapeDtypeStruct(group_block.shape, dtype)
    return pl.pallas_call(
        faces_kernel,
        out_shape=shape,
        in_specs=[pl.BlockSpec(memory_space=pltpu.SMEM)] + [vmem()] * (2 + len(slices)),
        out_specs=vmem(),
        name="faces",
    )(mix, prior, group_block, *slices)


def steps(surface, excitation, dtn_blocks, interp_blocks, adjacency):
    cols = lax.axis_size("col")
    rows = lax.axis_size("row")
    col = lax.axis_index("col")
    dtn = dtn_blocks[0]
    interp = interp_blocks[0]
    m, _ = interp.shape
    ms = m // cols
    n, ne = excitation.shape

    slices = []
    for k in range(cols):
        block = lax.dynamic_slice_in_dim(interp, ((col + k) & (cols - 1)) * ms, ms, 0)
        if k:
            block = lax.ppermute(block, "col", [(i, (i + k) % cols) for i in range(cols)])
        slices.append(block)

    adjacent = adjacency[0] % cols
    owners = jnp.arange(ne, dtype=jnp.int32)
    counts = jnp.sum((adjacent[None, :] == owners[:, None]).astype(F32), axis=1)
    me = (owners == col).astype(F32)
    weights = (1.0 + face_weight * NADJ) * me - face_weight * counts
    extra = jnp.broadcast_to(weights.astype(BF)[None, :], (16, ne))

    current = excitation
    residual = excitation
    mix = None
    for sweep in range(ITERS):
        rounded = current.astype(BF)
        piece = lax.ppermute(rounded, ("row", "col"), turned(rows, cols))
        column_block = copy_for_each(piece, "row").reshape(rows * n, ne)
        if sweep == 0:
            got = copy_for_each(jnp.concatenate([rounded, extra], axis=0), "col")
            group_block = got[:, :n].reshape(cols * n, ne)
            order = (col - jnp.arange(cols, dtype=jnp.int32)) & (cols - 1)
            pick = (order[:, None] == jnp.arange(cols, dtype=jnp.int32)[None, :]).astype(F32)
            mix = pick @ got[:, n, :cols].astype(F32) @ pick.T
        else:
            group_block = copy_for_each(rounded, "col").reshape(cols * n, ne)
        own = volume(interp, dtn, group_block)
        if sweep == 0:
            wide = applied(own, surface, column_block, F32)
            part = faces(mix, wide, group_block, slices, BF)
        else:
            wide = faces(mix, own, group_block, slices, F32)
            part = applied(wide, surface, column_block, BF)
        blocks = exchange(part.reshape(cols, n, ne), "col")
        summed = jnp.sum(blocks.astype(F32), axis=0)
        residual = excitation - current - summed
        current = current + damping * residual
    return (current, residual)


def solution(mesh):
    in_specs = (
        P("row", "col"),
        P(("row", "col"), None),
        P(("row", "col"), None, None),
        P(("row", "col"), None, None),
        P(("row", "col"), None),
    )
    out_specs = (P(("row", "col"), None), P(("row", "col"), None))
    return jax.shard_map(steps, mesh=mesh, in_specs=in_specs, out_specs=out_specs, check_vma=False)
```

```python
import jax
import jax.numpy as jnp
from jax import lax
from jax.experimental import pallas as pl
from jax.experimental.pallas import tpu as pltpu
from jax.sharding import PartitionSpec as P


ITERS = 2
NADJ = 6

damping = 0.25
face_weight = 0.25

BF = jnp.bfloat16
F32 = jnp.float32

PARAMS = pltpu.CompilerParams(vmem_limit_bytes=16 * 2**20)


def dot(a, b):
    return jnp.dot(a, b, preferred_element_type=F32)


def dot_t(a, b):
    return lax.dot_general(a, b, (((0,), (0,)), ((), ())), preferred_element_type=F32)


def exchange(blocks, axis):
    return lax.all_to_all(blocks, axis, split_axis=0, concat_axis=0, tiled=True)


def copy_for_each(shard, axis):
    return exchange(jnp.broadcast_to(shard, (lax.axis_size(axis), *shard.shape)), axis)


def turned(rows, cols):
    per_col = rows // cols
    return [
        (r * cols + c, ((r % per_col) * cols + c) * cols + r // per_col)
        for r in range(rows)
        for c in range(cols)
    ]


def volume_kernel(interp_ref, dtn_ref, group_ref, out_ref):
    traces = dot(interp_ref[...], group_ref[...]).astype(BF)
    response = dot(dtn_ref[...], traces).astype(BF)
    out_ref[...] = dot_t(interp_ref[...], response)


def faces_kernel(*refs):
    mix_ref, prior_ref, group_ref = refs[:3]
    slice_refs = refs[3:-1]
    out_ref = refs[-1]
    peers = len(slice_refs)
    group = group_ref[...]
    traces = [dot(ref[...], group).astype(BF).astype(F32) for ref in slice_refs]
    total = prior_ref[...]
    for s in range(peers):
        mixed = mix_ref[s, 0] * traces[0]
        for p in range(1, peers):
            mixed = mixed + mix_ref[s, p] * traces[p]
        total = total + dot_t(slice_refs[s][...], mixed.astype(BF))
    out_ref[...] = total.astype(out_ref.dtype)


def surface_kernel(prior_ref, surface_ref, column_ref, out_ref):
    out_ref[...] = (prior_ref[...] + dot(surface_ref[...], column_ref[...])).astype(out_ref.dtype)


def vmem():
    return pl.BlockSpec(memory_space=pltpu.VMEM)


def volume(interp, dtn, group_block):
    shape = jax.ShapeDtypeStruct(group_block.shape, F32)
    return pl.pallas_call(
        volume_kernel, out_shape=shape, in_specs=[vmem()] * 3, out_specs=vmem(), compiler_params=PARAMS, name="volume"
    )(interp, dtn, group_block)


def applied(prior, surface, column_block, dtype):
    shape = jax.ShapeDtypeStruct(prior.shape, dtype)
    return pl.pallas_call(
        surface_kernel, out_shape=shape, in_specs=[vmem()] * 3, out_specs=vmem(), compiler_params=PARAMS, name="applied"
    )(prior, surface, column_block)


def faces(mix, prior, group_block, slices, dtype):
    shape = jax.ShapeDtypeStruct(group_block.shape, dtype)
    return pl.pallas_call(
        faces_kernel,
        out_shape=shape,
        in_specs=[pl.BlockSpec(memory_space=pltpu.SMEM)] + [vmem()] * (2 + len(slices)),
        out_specs=vmem(),
        compiler_params=PARAMS,
        name="faces",
    )(mix, prior, group_block, *slices)


def steps(surface, excitation, dtn_blocks, interp_blocks, adjacency):
    cols = lax.axis_size("col")
    rows = lax.axis_size("row")
    col = lax.axis_index("col")
    dtn = dtn_blocks[0]
    interp = interp_blocks[0]
    m, _ = interp.shape
    ms = m // cols
    n, ne = excitation.shape

    slices = []
    for k in range(cols):
        block = lax.dynamic_slice_in_dim(interp, ((col + k) & (cols - 1)) * ms, ms, 0)
        if k:
            block = lax.ppermute(block, "col", [(i, (i + k) % cols) for i in range(cols)])
        slices.append(block)

    adjacent = adjacency[0] % cols
    owners = jnp.arange(ne, dtype=jnp.int32)
    counts = jnp.sum((adjacent[None, :] == owners[:, None]).astype(F32), axis=1)
    me = (owners == col).astype(F32)
    weights = (1.0 + face_weight * NADJ) * me - face_weight * counts
    extra = jnp.broadcast_to(weights.astype(BF)[None, :], (16, ne))

    current = excitation
    residual = excitation
    mix = None
    for sweep in range(ITERS):
        rounded = current.astype(BF)
        piece = lax.ppermute(rounded, ("row", "col"), turned(rows, cols))
        column_block = copy_for_each(piece, "row").reshape(rows * n, ne)
        if sweep == 0:
            got = copy_for_each(jnp.concatenate([rounded, extra], axis=0), "col")
            group_block = got[:, :n].reshape(cols * n, ne)
            order = (col - jnp.arange(cols, dtype=jnp.int32)) & (cols - 1)
            pick = (order[:, None] == jnp.arange(cols, dtype=jnp.int32)[None, :]).astype(F32)
            mix = pick @ got[:, n, :cols].astype(F32) @ pick.T
        else:
            group_block = copy_for_each(rounded, "col").reshape(cols * n, ne)
        own = volume(interp, dtn, group_block)
        if sweep == 0:
            wide = applied(own, surface, column_block, F32)
            part = faces(mix, wide, group_block, slices, BF)
        else:
            wide = faces(mix, own, group_block, slices, F32)
            part = applied(wide, surface, column_block, BF)
        blocks = exchange(part.reshape(cols, n, ne), "col")
        summed = jnp.sum(blocks.astype(F32), axis=0)
        residual = excitation - current - summed
        current = current + damping * residual
    return (current, residual)


def solution(mesh):
    in_specs = (
        P("row", "col"),
        P(("row", "col"), None),
        P(("row", "col"), None, None),
        P(("row", "col"), None, None),
        P(("row", "col"), None),
    )
    out_specs = (P(("row", "col"), None), P(("row", "col"), None))
    return jax.shard_map(steps, mesh=mesh, in_specs=in_specs, out_specs=out_specs, check_vma=False)
```

```python
import jax
import jax.numpy as jnp
from jax import lax
from jax.experimental import pallas as pl
from jax.experimental.pallas import tpu as pltpu
from jax.sharding import PartitionSpec as P


ITERS = 2
NADJ = 6

damping = 0.25
face_weight = 0.25

BF = jnp.bfloat16
F32 = jnp.float32

PARAMS = pltpu.CompilerParams(vmem_limit_bytes=16 * 2**20)


def dot(a, b):
    return jnp.dot(a, b, preferred_element_type=F32)


def dot_t(a, b):
    return lax.dot_general(a, b, (((0,), (0,)), ((), ())), preferred_element_type=F32)


def exchange(blocks, axis):
    return lax.all_to_all(blocks, axis, split_axis=0, concat_axis=0, tiled=True)


def copy_for_each(shard, axis):
    return exchange(jnp.broadcast_to(shard, (lax.axis_size(axis), *shard.shape)), axis)


def turned(rows, cols):
    per_col = rows // cols
    return [
        (r * cols + c, ((r % per_col) * cols + c) * cols + r // per_col)
        for r in range(rows)
        for c in range(cols)
    ]


def rotated(col, k, peers):
    return (col + k) & (peers - 1)


def grouped(got_ref, n):
    got = got_ref[:, :n]
    return got.reshape(got.shape[0] * n, got.shape[2])


def volume_kernel(interp_ref, dtn_ref, got_ref, *refs):
    peers = got_ref.shape[0]
    traces = dot(interp_ref[...], grouped(got_ref, interp_ref.shape[1] // peers)).astype(BF)
    response = dot(dtn_ref[...], traces).astype(BF)
    total = dot_t(interp_ref[...], response)
    if len(refs) == 2:
        total = total + refs[0][...]
    refs[-1][...] = total


def faces_kernel(col_ref, mix_ref, got_ref, *refs):
    peers = got_ref.shape[0]
    slice_refs, prior_refs = refs[:peers], refs[peers:-2]
    out_ref, traces_ref = refs[-2:]
    n = slice_refs[0].shape[1] // peers
    group = grouped(got_ref, n)
    for k in range(peers):
        traces_ref[rotated(col_ref[0], -k, peers)] = dot(slice_refs[k][...], group)
    total = prior_refs[0][...] if prior_refs else None
    for k in range(peers):
        s = rotated(col_ref[0], -k, peers)
        row = mix_ref[s, n : n + 16, :].astype(F32)[:1]
        mixed = None
        for p in range(peers):
            term = row[:, p : p + 1] * traces_ref[p]
            mixed = term if mixed is None else mixed + term
        term = dot_t(slice_refs[k][...], mixed.astype(BF))
        total = term if total is None else total + term
    out_ref[...] = total.astype(out_ref.dtype)


def surface_kernel(prior_ref, surface_ref, column_ref, out_ref):
    out_ref[...] = (prior_ref[...] + dot(surface_ref[...], column_ref[...])).astype(out_ref.dtype)


def vmem():
    return pl.BlockSpec(memory_space=pltpu.VMEM)


def cost(products, m, k, ne):
    return pl.CostEstimate(
        flops=2 * products * m * k * ne, bytes_accessed=2 * products * m * k, transcendentals=0
    )


def volume(interp, dtn, got, *prior):
    m, rb = interp.shape
    ne = got.shape[-1]
    return pl.pallas_call(
        volume_kernel,
        out_shape=jax.ShapeDtypeStruct((rb, ne), F32),
        in_specs=[vmem()] * (3 + len(prior)),
        out_specs=vmem(),
        compiler_params=PARAMS,
        cost_estimate=cost(3, m, rb, ne),
        name="volume",
    )(interp, dtn, got, *prior)


def applied(prior, surface, column_block, dtype):
    m, k = surface.shape
    return pl.pallas_call(
        surface_kernel,
        out_shape=jax.ShapeDtypeStruct(prior.shape, dtype),
        in_specs=[vmem()] * 3,
        out_specs=vmem(),
        compiler_params=PARAMS,
        cost_estimate=cost(1, m, k, prior.shape[1]),
        name="applied",
    )(prior, surface, column_block)


def faces(place, mix, got, slices, dtype, *prior):
    (ms, rb), ne = slices[0].shape, got.shape[-1]
    peers = len(slices)
    return pl.pallas_call(
        faces_kernel,
        out_shape=jax.ShapeDtypeStruct((rb, ne), dtype),
        in_specs=[pl.BlockSpec(memory_space=pltpu.SMEM)] + [vmem()] * (2 + peers + len(prior)),
        out_specs=vmem(),
        scratch_shapes=[pltpu.VMEM((peers, ms, ne), F32)],
        compiler_params=PARAMS,
        cost_estimate=cost(2, peers * ms, rb, ne),
        name="faces",
    )(place, mix, got, *slices, *prior)


def steps(surface, excitation, dtn_blocks, interp_blocks, adjacency):
    cols = lax.axis_size("col")
    rows = lax.axis_size("row")
    col = lax.axis_index("col")
    place = col.astype(jnp.int32)[None]
    dtn = dtn_blocks[0]
    interp = interp_blocks[0]
    ms = interp.shape[0] // cols
    n, ne = excitation.shape

    slices = []
    for k in range(cols):
        block = lax.dynamic_slice_in_dim(interp, rotated(col, k, cols) * ms, ms, 0)
        if k:
            block = lax.ppermute(block, "col", [(i, (i + k) % cols) for i in range(cols)])
        slices.append(block)

    adjacent = adjacency[0] & (cols - 1)
    owners = jnp.arange(ne, dtype=jnp.int32)
    counts = jnp.sum((adjacent[None, :] == owners[:, None]).astype(F32), axis=1)
    me = (owners == col).astype(F32)
    weights = (1.0 + face_weight * NADJ) * me - face_weight * counts
    extra = jnp.broadcast_to(weights.astype(BF)[None, :], (16, ne))

    current = excitation
    residual = excitation
    mix = None
    for sweep in range(ITERS):
        rounded = current.astype(BF)
        piece = lax.ppermute(rounded, ("row", "col"), turned(rows, cols))
        column_block = copy_for_each(piece, "row").reshape(rows * n, ne)
        sent = jnp.concatenate([rounded, extra], axis=0) if sweep == 0 else rounded
        got = copy_for_each(sent, "col")
        mix = got if mix is None else mix
        if sweep == 0:
            own = volume(interp, dtn, got)
            wide = applied(own, surface, column_block, F32)
            part = faces(place, mix, got, slices, BF, wide)
        else:
            wide = faces(place, mix, got, slices, F32)
            own = volume(interp, dtn, got, wide)
            part = applied(own, surface, column_block, BF)
        parts = exchange(part.reshape(cols, n, ne), "col")
        summed = jnp.sum(parts.astype(F32), axis=0)
        residual = excitation - current - summed
        current = current + damping * residual
    return (current, residual)


def solution(mesh):
    in_specs = (
        P("row", "col"),
        P(("row", "col"), None),
        P(("row", "col"), None, None),
        P(("row", "col"), None, None),
        P(("row", "col"), None),
    )
    out_specs = (P(("row", "col"), None), P(("row", "col"), None))
    return jax.shard_map(steps, mesh=mesh, in_specs=in_specs, out_specs=out_specs, check_vma=False)
```

```python
import functools

import jax
import jax.numpy as jnp
from jax import lax
from jax.experimental import pallas as pl
from jax.experimental.pallas import tpu as pltpu
from jax.sharding import PartitionSpec as P


ITERS = 2
NADJ = 6

damping = 0.25
face_weight = 0.25

BF = jnp.bfloat16
F32 = jnp.float32

PARAMS = pltpu.CompilerParams(vmem_limit_bytes=16 * 2**20)


def dot(a, b):
    return jnp.dot(a, b, preferred_element_type=F32)


def dot_t(a, b):
    return lax.dot_general(a, b, (((0,), (0,)), ((), ())), preferred_element_type=F32)


def exchange(blocks, axis):
    return lax.all_to_all(blocks, axis, split_axis=0, concat_axis=0, tiled=True)


def copy_for_each(shard, axis):
    return exchange(jnp.broadcast_to(shard, (lax.axis_size(axis), *shard.shape)), axis)


def turned(rows, cols):
    per_col = rows // cols
    return [
        (r * cols + c, ((r % per_col) * cols + c) * cols + r // per_col)
        for r in range(rows)
        for c in range(cols)
    ]


def rotated(col, k, peers):
    return (col + k) & (peers - 1)


def owner(col, distance, j, peers):
    return rotated(col, -2 * distance, peers) ^ j


def assemble_kernel(outs, col_ref, *refs):
    pair_refs, group_ref = refs[:-outs], refs[-outs]
    peers = 2 * len(pair_refs)
    n = group_ref.shape[0] // peers
    for d, pair_ref in enumerate(pair_refs):
        for j in range(2):
            s = owner(col_ref[0], d, j, peers)
            group_ref[pl.ds(pl.multiple_of(s * n, n), n), :] = pair_ref[j, :n, :]
            if outs == 2:
                refs[-1][s] = pair_ref[j, n:, :].astype(F32)


def volume_kernel(interp_ref, dtn_ref, group_ref, *refs):
    traces = dot(interp_ref[...], group_ref[...]).astype(BF)
    response = dot(dtn_ref[...], traces).astype(BF)
    total = dot_t(interp_ref[...], response)
    if len(refs) == 2:
        total = total + refs[0][...]
    refs[-1][...] = total


def faces_kernel(col_ref, mix_ref, group_ref, *refs):
    peers = mix_ref.shape[0]
    slice_refs, prior_refs = refs[:peers], refs[peers:-2]
    out_ref, traces_ref = refs[-2:]
    group = group_ref[...]
    for k in range(peers):
        traces_ref[rotated(col_ref[0], -k, peers)] = dot(slice_refs[k][...], group)
    total = prior_refs[0][...] if prior_refs else None
    for k in range(peers):
        row = mix_ref[rotated(col_ref[0], -k, peers)][:1]
        mixed = None
        for p in range(peers):
            term = row[:, p : p + 1] * traces_ref[p]
            mixed = term if mixed is None else mixed + term
        term = dot_t(slice_refs[k][...], mixed.astype(BF))
        total = term if total is None else total + term
    out_ref[...] = total.astype(out_ref.dtype)


def surface_kernel(prior_ref, surface_ref, column_ref, out_ref):
    out_ref[...] = (prior_ref[...] + dot(surface_ref[...], column_ref[...])).astype(out_ref.dtype)


def vmem():
    return pl.BlockSpec(memory_space=pltpu.VMEM)


def cost(products, m, k, ne):
    return pl.CostEstimate(
        flops=2 * products * m * k * ne, bytes_accessed=2 * products * m * k, transcendentals=0
    )


def smem():
    return pl.BlockSpec(memory_space=pltpu.SMEM)


def assemble(place, pairs, n):
    peers, (_, high, ne) = 2 * len(pairs), pairs[0].shape
    shapes = [jax.ShapeDtypeStruct((peers * n, ne), BF)]
    if high > n:
        shapes.append(jax.ShapeDtypeStruct((peers, high - n, ne), F32))
    return pl.pallas_call(
        functools.partial(assemble_kernel, len(shapes)),
        out_shape=shapes,
        in_specs=[smem()] + [vmem()] * len(pairs),
        out_specs=[vmem()] * len(shapes),
        compiler_params=PARAMS,
        name="assemble",
    )(place, *pairs)


def volume(interp, dtn, group, *prior):
    m, rb = interp.shape
    ne = group.shape[-1]
    return pl.pallas_call(
        volume_kernel,
        out_shape=jax.ShapeDtypeStruct((rb, ne), F32),
        in_specs=[vmem()] * (3 + len(prior)),
        out_specs=vmem(),
        compiler_params=PARAMS,
        cost_estimate=cost(3, m, rb, ne),
        name="volume",
    )(interp, dtn, group, *prior)


def applied(prior, surface, column_block, dtype):
    m, k = surface.shape
    return pl.pallas_call(
        surface_kernel,
        out_shape=jax.ShapeDtypeStruct(prior.shape, dtype),
        in_specs=[vmem()] * 3,
        out_specs=vmem(),
        compiler_params=PARAMS,
        cost_estimate=cost(1, m, k, prior.shape[1]),
        name="applied",
    )(prior, surface, column_block)


def faces(place, mix, group, slices, dtype, *prior):
    (ms, rb), ne = slices[0].shape, group.shape[-1]
    peers = len(slices)
    return pl.pallas_call(
        faces_kernel,
        out_shape=jax.ShapeDtypeStruct((rb, ne), dtype),
        in_specs=[smem()] + [vmem()] * (2 + peers + len(prior)),
        out_specs=vmem(),
        scratch_shapes=[pltpu.VMEM((peers, ms, ne), F32)],
        compiler_params=PARAMS,
        cost_estimate=cost(2, peers * ms, rb, ne),
        name="faces",
    )(place, mix, group, *slices, *prior)


def gathered(shard, cols):
    other = lax.ppermute(shard, "col", [(i, i ^ 1) for i in range(cols)])
    pair = jnp.stack([shard, other])
    pairs = [pair]
    for d in range(1, cols // 2):
        path = [(i, (i + 2 * d) % cols) for i in range(cols)]
        pairs.append(lax.ppermute(pair, "col", path))
    return pairs


def steps(surface, excitation, dtn_blocks, interp_blocks, adjacency):
    cols = lax.axis_size("col")
    rows = lax.axis_size("row")
    col = lax.axis_index("col")
    place = col.astype(jnp.int32)[None]
    dtn = dtn_blocks[0]
    interp = interp_blocks[0]
    ms = interp.shape[0] // cols
    n, ne = excitation.shape

    slices = []
    for k in range(cols):
        block = lax.dynamic_slice_in_dim(interp, rotated(col, k, cols) * ms, ms, 0)
        if k:
            block = lax.ppermute(block, "col", [(i, (i + k) % cols) for i in range(cols)])
        slices.append(block)

    adjacent = adjacency[0] & (cols - 1)
    owners = jnp.arange(ne, dtype=jnp.int32)
    counts = jnp.sum((adjacent[None, :] == owners[:, None]).astype(F32), axis=1)
    me = (owners == col).astype(F32)
    weights = (1.0 + face_weight * NADJ) * me - face_weight * counts
    extra = jnp.broadcast_to(weights.astype(BF)[None, :], (16, ne))

    current = excitation
    residual = excitation
    mix = None
    for sweep in range(ITERS):
        rounded = current.astype(BF)
        piece = lax.ppermute(rounded, ("row", "col"), turned(rows, cols))
        column_block = copy_for_each(piece, "row").reshape(rows * n, ne)
        sent = jnp.concatenate([rounded, extra], axis=0) if sweep == 0 else rounded
        pairs = gathered(sent, cols)
        group, *rows_got = assemble(place, pairs, n)
        if sweep == 0:
            mix = rows_got[0]
            own = volume(interp, dtn, group)
            wide = applied(own, surface, column_block, F32)
            part = faces(place, mix, group, slices, BF, wide)
        else:
            wide = faces(place, mix, group, slices, F32)
            own = volume(interp, dtn, group, wide)
            part = applied(own, surface, column_block, BF)
        parts = exchange(part.reshape(cols, n, ne), "col")
        summed = jnp.sum(parts.astype(F32), axis=0)
        residual = excitation - current - summed
        current = current + damping * residual
    return (current, residual)


def solution(mesh):
    in_specs = (
        P("row", "col"),
        P(("row", "col"), None),
        P(("row", "col"), None, None),
        P(("row", "col"), None, None),
        P(("row", "col"), None),
    )
    out_specs = (P(("row", "col"), None), P(("row", "col"), None))
    return jax.shard_map(steps, mesh=mesh, in_specs=in_specs, out_specs=out_specs, check_vma=False)
```

```python
import functools

import jax
import jax.numpy as jnp
from jax import lax
from jax.experimental import pallas as pl
from jax.experimental.pallas import tpu as pltpu
from jax.sharding import PartitionSpec as P


ITERS = 2
NADJ = 6

damping = 0.25
face_weight = 0.25

BF = jnp.bfloat16
F32 = jnp.float32

PARAMS = pltpu.CompilerParams(vmem_limit_bytes=16 * 2**20)


def dot(a, b):
    return jnp.dot(a, b, preferred_element_type=F32)


def dot_t(a, b):
    return lax.dot_general(a, b, (((0,), (0,)), ((), ())), preferred_element_type=F32)


def exchange(blocks, axis):
    return lax.all_to_all(blocks, axis, split_axis=0, concat_axis=0, tiled=True)


def copy_for_each(shard, axis):
    return exchange(jnp.broadcast_to(shard, (lax.axis_size(axis), *shard.shape)), axis)


def turned(rows, cols):
    per_col = rows // cols
    return [
        (r * cols + c, ((r % per_col) * cols + c) * cols + r // per_col)
        for r in range(rows)
        for c in range(cols)
    ]


def rotated(col, k, peers):
    return (col + k) & (peers - 1)


def owner(col, distance, j, peers):
    return rotated(col, -2 * distance, peers) ^ j


def assemble_kernel(outs, col_ref, *refs):
    pair_refs, group_ref = refs[:-outs], refs[-outs]
    peers = 2 * len(pair_refs)
    n = group_ref.shape[0] // peers
    for d, pair_ref in enumerate(pair_refs):
        for j in range(2):
            s = owner(col_ref[0], d, j, peers)
            group_ref[pl.ds(pl.multiple_of(s * n, n), n), :] = pair_ref[j, :n, :]
            if outs == 2:
                refs[-1][s] = pair_ref[j, n:, :].astype(F32)


def volume_kernel(interp_ref, dtn_ref, group_ref, *refs):
    traces = dot(interp_ref[...], group_ref[...]).astype(BF)
    response = dot(dtn_ref[...], traces).astype(BF)
    total = dot_t(interp_ref[...], response)
    if len(refs) == 2:
        total = total + refs[0][...]
    refs[-1][...] = total


def faces_kernel(has_prior, col_ref, mix_ref, group_ref, *refs):
    peers = mix_ref.shape[0]
    slice_refs, prior_refs = refs[:peers], refs[peers : peers + has_prior]
    out_refs, traces_ref = refs[peers + has_prior : -1], refs[-1]
    group = group_ref[...]
    for k in range(peers):
        traces_ref[rotated(col_ref[0], -k, peers)] = dot(slice_refs[k][...], group)
    total = prior_refs[0][...] if prior_refs else None
    for k in range(peers):
        row = mix_ref[rotated(col_ref[0], -k, peers)][:1]
        mixed = None
        for p in range(peers):
            term = row[:, p : p + 1] * traces_ref[p]
            mixed = term if mixed is None else mixed + term
        term = dot_t(slice_refs[k][...], mixed.astype(BF))
        total = term if total is None else total + term
    if len(out_refs) == 1:
        out_refs[0][...] = total
    else:
        divide(col_ref[0], total, traces_ref, *out_refs)


def divide(col, total, blocks_ref, keep_ref, give_ref):
    peers, n, ne = blocks_ref.shape
    blocks_ref[...] = total.reshape(peers, n, ne)
    for d in range(peers // 2):
        keep_ref[d] = blocks_ref[rotated(col, 2 * d, peers)]
        give_ref[d] = blocks_ref[rotated(col, 2 * d, peers) ^ 1].astype(BF)


def surface_kernel(col_ref, prior_ref, surface_ref, column_ref, *refs):
    total = prior_ref[...] + dot(surface_ref[...], column_ref[...])
    if len(refs) == 1:
        refs[0][...] = total
    else:
        divide(col_ref[0], total, refs[2], *refs[:2])


def divided(peers, shape):
    n, ne = shape[0] // peers, shape[1]
    return [
        jax.ShapeDtypeStruct((peers // 2, n, ne), F32),
        jax.ShapeDtypeStruct((peers // 2, n, ne), BF),
    ]


def vmem():
    return pl.BlockSpec(memory_space=pltpu.VMEM)


def cost(products, m, k, ne):
    return pl.CostEstimate(
        flops=2 * products * m * k * ne, bytes_accessed=2 * products * m * k, transcendentals=0
    )


def smem():
    return pl.BlockSpec(memory_space=pltpu.SMEM)


def assemble(place, pairs, n):
    peers, (_, high, ne) = 2 * len(pairs), pairs[0].shape
    shapes = [jax.ShapeDtypeStruct((peers * n, ne), BF)]
    if high > n:
        shapes.append(jax.ShapeDtypeStruct((peers, high - n, ne), F32))
    return pl.pallas_call(
        functools.partial(assemble_kernel, len(shapes)),
        out_shape=shapes,
        in_specs=[smem()] + [vmem()] * len(pairs),
        out_specs=[vmem()] * len(shapes),
        compiler_params=PARAMS,
        name="assemble",
    )(place, *pairs)


def volume(interp, dtn, group, *prior):
    m, rb = interp.shape
    ne = group.shape[-1]
    return pl.pallas_call(
        volume_kernel,
        out_shape=jax.ShapeDtypeStruct((rb, ne), F32),
        in_specs=[vmem()] * (3 + len(prior)),
        out_specs=vmem(),
        compiler_params=PARAMS,
        cost_estimate=cost(3, m, rb, ne),
        name="volume",
    )(interp, dtn, group, *prior)


def applied(place, prior, surface, column_block, peers=0):
    (m, k), ne = surface.shape, prior.shape[1]
    plain = [jax.ShapeDtypeStruct(prior.shape, F32)]
    shapes = divided(peers, prior.shape) if peers else plain
    return pl.pallas_call(
        surface_kernel,
        out_shape=shapes,
        in_specs=[smem()] + [vmem()] * 3,
        out_specs=[vmem()] * len(shapes),
        scratch_shapes=[pltpu.VMEM((peers, m // peers, ne), F32)] if peers else [],
        compiler_params=PARAMS,
        cost_estimate=cost(1, m, k, ne),
        name="applied",
    )(place, prior, surface, column_block)


def faces(place, mix, group, slices, *prior):
    (ms, rb), ne = slices[0].shape, group.shape[-1]
    peers = len(slices)
    plain = [jax.ShapeDtypeStruct((rb, ne), F32)]
    shapes = divided(peers, (rb, ne)) if prior else plain
    return pl.pallas_call(
        functools.partial(faces_kernel, len(prior)),
        out_shape=shapes,
        in_specs=[smem()] + [vmem()] * (2 + peers + len(prior)),
        out_specs=[vmem()] * len(shapes),
        scratch_shapes=[pltpu.VMEM((peers, ms, ne), F32)],
        compiler_params=PARAMS,
        cost_estimate=cost(2, peers * ms, rb, ne),
        name="faces",
    )(place, mix, group, *slices, *prior)


def swapped(shard, cols):
    return lax.ppermute(shard, "col", [(i, i ^ 1) for i in range(cols)])


def along(shard, d, cols):
    return lax.ppermute(shard, "col", [(i, (i + 2 * d) % cols) for i in range(cols)])


def summed_over(keep, give, cols):
    taken = swapped(give, cols)
    sums = keep + taken.astype(F32)
    total = sums[0]
    for d in range(1, cols // 2):
        total = total + along(sums[d].astype(BF), d, cols).astype(F32)
    return total


def gathered(shard, cols):
    other = swapped(shard, cols)
    pair = jnp.stack([shard, other])
    pairs = [pair]
    for d in range(1, cols // 2):
        pairs.append(along(pair, d, cols))
    return pairs


def steps(surface, excitation, dtn_blocks, interp_blocks, adjacency):
    cols = lax.axis_size("col")
    rows = lax.axis_size("row")
    col = lax.axis_index("col")
    place = col.astype(jnp.int32)[None]
    dtn = dtn_blocks[0]
    interp = interp_blocks[0]
    ms = interp.shape[0] // cols
    n, ne = excitation.shape

    slices = []
    for k in range(cols):
        block = lax.dynamic_slice_in_dim(interp, rotated(col, k, cols) * ms, ms, 0)
        if k:
            block = lax.ppermute(block, "col", [(i, (i + k) % cols) for i in range(cols)])
        slices.append(block)

    adjacent = adjacency[0] & (cols - 1)
    owners = jnp.arange(ne, dtype=jnp.int32)
    counts = jnp.sum((adjacent[None, :] == owners[:, None]).astype(F32), axis=1)
    me = (owners == col).astype(F32)
    weights = (1.0 + face_weight * NADJ) * me - face_weight * counts
    extra = jnp.broadcast_to(weights.astype(BF)[None, :], (16, ne))

    current = excitation
    residual = excitation
    mix = None
    for sweep in range(ITERS):
        rounded = current.astype(BF)
        piece = lax.ppermute(rounded, ("row", "col"), turned(rows, cols))
        column_block = copy_for_each(piece, "row").reshape(rows * n, ne)
        sent = jnp.concatenate([rounded, extra], axis=0) if sweep == 0 else rounded
        pairs = gathered(sent, cols)
        group, *rows_got = assemble(place, pairs, n)
        if sweep == 0:
            mix = rows_got[0]
            own = volume(interp, dtn, group)
            wide = applied(place, own, surface, column_block)[0]
            keep, give = faces(place, mix, group, slices, wide)
        else:
            wide = faces(place, mix, group, slices)[0]
            own = volume(interp, dtn, group, wide)
            keep, give = applied(place, own, surface, column_block, cols)
        summed = summed_over(keep, give, cols)
        residual = excitation - current - summed
        current = current + damping * residual
    return (current, residual)


def solution(mesh):
    in_specs = (
        P("row", "col"),
        P(("row", "col"), None),
        P(("row", "col"), None, None),
        P(("row", "col"), None, None),
        P(("row", "col"), None),
    )
    out_specs = (P(("row", "col"), None), P(("row", "col"), None))
    return jax.shard_map(steps, mesh=mesh, in_specs=in_specs, out_specs=out_specs, check_vma=False)
```

```python
import functools

import jax
import jax.numpy as jnp
from jax import lax
from jax.experimental import pallas as pl
from jax.experimental.pallas import tpu as pltpu
from jax.sharding import PartitionSpec as P


ITERS = 2
NADJ = 6

damping = 0.25
face_weight = 0.25

BF = jnp.bfloat16
F32 = jnp.float32

PARAMS = pltpu.CompilerParams(vmem_limit_bytes=16 * 2**20)


def dot(a, b):
    return jnp.dot(a, b, preferred_element_type=F32)


def dot_t(a, b):
    return lax.dot_general(a, b, (((0,), (0,)), ((), ())), preferred_element_type=F32)


def exchange(blocks, axis):
    return lax.all_to_all(blocks, axis, split_axis=0, concat_axis=0, tiled=True)


def copy_for_each(shard, axis):
    return exchange(jnp.broadcast_to(shard, (lax.axis_size(axis), *shard.shape)), axis)


def turned(rows, cols):
    per_col = rows // cols
    return [
        (r * cols + c, ((r % per_col) * cols + c) * cols + r // per_col)
        for r in range(rows)
        for c in range(cols)
    ]


def rotated(col, k, peers):
    return (col + k) & (peers - 1)


def owner(col, distance, j, peers):
    return rotated(col, -2 * distance, peers) ^ j


def assemble_kernel(count, outs, col_ref, *refs):
    pair_refs, group_ref = refs[:count], refs[-outs]
    peers = 2 * len(pair_refs)
    n = group_ref.shape[0] // peers
    for d, pair_ref in enumerate(pair_refs):
        for j in range(2):
            s = owner(col_ref[0], d, j, peers)
            group_ref[pl.ds(pl.multiple_of(s * n, n), n), :] = pair_ref[j, :n, :]
            if outs == 2:
                refs[-1][s] = pair_ref[j, n:, :].astype(F32)


def volume_kernel(has_prior, interp_ref, dtn_ref, group_ref, *refs):
    traces = dot(interp_ref[...], group_ref[...]).astype(BF)
    response = dot(dtn_ref[...], traces).astype(BF)
    total = dot_t(interp_ref[...], response)
    if has_prior:
        total = total + refs[0][...]
    refs[-1][...] = total


def faces_kernel(has_prior, col_ref, mix_ref, group_ref, *refs):
    peers = mix_ref.shape[0]
    slice_refs, prior_refs = refs[:peers], refs[peers : peers + has_prior]
    out_refs, traces_ref = refs[peers + has_prior : -1], refs[-1]
    group = group_ref[...]
    for k in range(peers):
        traces_ref[rotated(col_ref[0], -k, peers)] = dot(slice_refs[k][...], group)
    total = prior_refs[0][...] if prior_refs else None
    for k in range(peers):
        row = mix_ref[rotated(col_ref[0], -k, peers)][:1]
        mixed = None
        for p in range(peers):
            term = row[:, p : p + 1] * traces_ref[p]
            mixed = term if mixed is None else mixed + term
        term = dot_t(slice_refs[k][...], mixed.astype(BF))
        total = term if total is None else total + term
    if len(out_refs) == 1:
        out_refs[0][...] = total
    else:
        divide(col_ref[0], total, traces_ref, *out_refs)


def divide(col, total, blocks_ref, keep_ref, give_ref):
    peers, n, ne = blocks_ref.shape
    blocks_ref[...] = total.reshape(peers, n, ne)
    for d in range(peers // 2):
        keep_ref[d] = blocks_ref[col ^ (2 * d)]
        give_ref[d] = blocks_ref[col ^ (2 * d + 1)].astype(BF)


def surface_kernel(col_ref, prior_ref, surface_ref, column_ref, *refs):
    total = prior_ref[...] + dot(surface_ref[...], column_ref[...])
    if len(refs) == 1:
        refs[0][...] = total
    else:
        divide(col_ref[0], total, refs[2], *refs[:2])


def streamed_kernel(col_ref, prior_ref, surface_ref, column_ref, *refs):
    keep_ref, give_ref, blocks_ref, parts_ref, sems = refs
    pieces, high, _ = parts_ref.shape
    copies = [
        pltpu.make_async_copy(
            surface_ref.at[pl.ds(p * high, high)], parts_ref.at[p], sems.at[p]
        )
        for p in range(pieces)
    ]
    for copy in copies:
        copy.start()
    column = column_ref[...]
    each, n, ne = high // blocks_ref.shape[1], blocks_ref.shape[1], blocks_ref.shape[2]
    for p, copy in enumerate(copies):
        copy.wait()
        total = prior_ref[pl.ds(p * high, high), :] + dot(parts_ref[p], column)
        blocks_ref[pl.ds(p * each, each)] = total.reshape(each, n, ne)
    for d in range(blocks_ref.shape[0] // 2):
        keep_ref[d] = blocks_ref[col_ref[0] ^ (2 * d)]
        give_ref[d] = blocks_ref[col_ref[0] ^ (2 * d + 1)].astype(BF)


def streamed(place, prior, surface, column_block, peers, pieces=4):
    (m, k), ne = surface.shape, prior.shape[1]
    shapes = divided(peers, prior.shape)
    return pl.pallas_call(
        streamed_kernel,
        out_shape=shapes,
        in_specs=[smem(), vmem(), hbm(), vmem()],
        out_specs=[vmem()] * len(shapes),
        scratch_shapes=[
            pltpu.VMEM((peers, m // peers, ne), F32),
            pltpu.VMEM((pieces, m // pieces, k), BF),
            pltpu.SemaphoreType.DMA((pieces,)),
        ],
        compiler_params=pltpu.CompilerParams(vmem_limit_bytes=60 * 2**20),
        name="streamed",
    )(place, prior, surface, column_block)


def divided(peers, shape):
    n, ne = shape[0] // peers, shape[1]
    return [
        jax.ShapeDtypeStruct((peers // 2, n, ne), F32),
        jax.ShapeDtypeStruct((peers // 2, n, ne), BF),
    ]


def vmem():
    return pl.BlockSpec(memory_space=pltpu.VMEM)


def hbm():
    return pl.BlockSpec(memory_space=pl.ANY)


def cost(products, m, k, ne):
    return pl.CostEstimate(
        flops=2 * products * m * k * ne, bytes_accessed=2 * products * m * k, transcendentals=0
    )


def smem():
    return pl.BlockSpec(memory_space=pltpu.SMEM)


def assemble(place, pairs, n, held):
    peers, (_, high, ne) = 2 * len(pairs), pairs[0].shape
    shapes = [jax.ShapeDtypeStruct((peers * n, ne), BF)]
    if high > n:
        shapes.append(jax.ShapeDtypeStruct((peers, high - n, ne), F32))
    return pl.pallas_call(
        functools.partial(assemble_kernel, len(pairs), len(shapes)),
        out_shape=shapes,
        in_specs=[smem()] + [vmem()] * len(pairs) + [hbm()] * len(held),
        out_specs=[vmem()] * len(shapes),
        compiler_params=PARAMS,
        cost_estimate=cost(1, 256, 1024, 1),
        name="assemble",
    )(place, *pairs, *held)


def volume(interp, dtn, group, prior=(), held=()):
    m, rb = interp.shape
    ne = group.shape[-1]
    return pl.pallas_call(
        functools.partial(volume_kernel, len(prior)),
        out_shape=jax.ShapeDtypeStruct((rb, ne), F32),
        in_specs=[vmem()] * (3 + len(prior) + len(held)),
        out_specs=vmem(),
        compiler_params=PARAMS,
        cost_estimate=cost(3, m, rb, ne),
        name="volume",
    )(interp, dtn, group, *prior, *held)


def applied(place, prior, surface, column_block, peers=0):
    (m, k), ne = surface.shape, prior.shape[1]
    plain = [jax.ShapeDtypeStruct(prior.shape, F32)]
    shapes = divided(peers, prior.shape) if peers else plain
    return pl.pallas_call(
        surface_kernel,
        out_shape=shapes,
        in_specs=[smem()] + [vmem()] * 3,
        out_specs=[vmem()] * len(shapes),
        scratch_shapes=[pltpu.VMEM((peers, m // peers, ne), F32)] if peers else [],
        compiler_params=PARAMS,
        cost_estimate=cost(1, m, k, ne),
        name="applied",
    )(place, prior, surface, column_block)


def faces(place, mix, group, slices, *prior):
    (ms, rb), ne = slices[0].shape, group.shape[-1]
    peers = len(slices)
    plain = [jax.ShapeDtypeStruct((rb, ne), F32)]
    shapes = divided(peers, (rb, ne)) if prior else plain
    return pl.pallas_call(
        functools.partial(faces_kernel, len(prior)),
        out_shape=shapes,
        in_specs=[smem()] + [vmem()] * (2 + peers + len(prior)),
        out_specs=[vmem()] * len(shapes),
        scratch_shapes=[pltpu.VMEM((peers, ms, ne), F32)],
        compiler_params=PARAMS,
        cost_estimate=cost(2, peers * ms, rb, ne),
        name="faces",
    )(place, mix, group, *slices, *prior)


def swapped(shard, cols, bits=1):
    return lax.ppermute(shard, "col", [(i, i ^ bits) for i in range(cols)])


def along(shard, d, cols):
    return lax.ppermute(shard, "col", [(i, (i + 2 * d) % cols) for i in range(cols)])


def summed_over(keep, give, cols):
    taken = swapped(give, cols)
    sums = keep + taken.astype(F32)
    taken = swapped(sums[1:3].astype(BF), cols, 2).astype(F32)
    last = swapped((sums[3] + taken[1]).astype(BF), cols, 6).astype(F32)
    return sums[0] + taken[0] + last


def gathered(shard, cols):
    other = swapped(shard, cols)
    pair = jnp.stack([shard, other])
    pairs = [pair]
    for d in range(1, cols // 2):
        pairs.append(along(pair, d, cols))
    return pairs


def steps(surface, excitation, dtn_blocks, interp_blocks, adjacency):
    cols = lax.axis_size("col")
    rows = lax.axis_size("row")
    col = lax.axis_index("col")
    place = col.astype(jnp.int32)[None]
    dtn = dtn_blocks[0]
    interp = interp_blocks[0]
    ms = interp.shape[0] // cols
    n, ne = excitation.shape

    slices = []
    for k in range(cols):
        block = lax.dynamic_slice_in_dim(interp, rotated(col, k, cols) * ms, ms, 0)
        if k:
            block = lax.ppermute(block, "col", [(i, (i + k) % cols) for i in range(cols)])
        slices.append(block)

    adjacent = adjacency[0] & (cols - 1)
    owners = jnp.arange(ne, dtype=jnp.int32)
    counts = jnp.sum((adjacent[None, :] == owners[:, None]).astype(F32), axis=1)
    me = (owners == col).astype(F32)
    weights = (1.0 + face_weight * NADJ) * me - face_weight * counts
    extra = jnp.broadcast_to(weights.astype(BF)[None, :], (16, ne))

    current = excitation
    residual = excitation
    mix = None
    for sweep in range(ITERS):
        rounded = current.astype(BF)
        piece = lax.ppermute(rounded, ("row", "col"), turned(rows, cols))
        column_block = copy_for_each(piece, "row").reshape(rows * n, ne)
        sent = jnp.concatenate([rounded, extra], axis=0) if sweep == 0 else rounded
        pairs = gathered(sent, cols)
        group, *rows_got = assemble(place, pairs, n, () if sweep else (column_block,))
        if sweep == 0:
            mix = rows_got[0]
            own = volume(interp, dtn, group)
            wide = applied(place, own, surface, column_block)[0]
            keep, give = faces(place, mix, group, slices, wide)
        else:
            wide = faces(place, mix, group, slices)[0]
            own = volume(interp, dtn, group, (wide,))
            keep, give = streamed(place, own, surface, column_block, cols)
        summed = summed_over(keep, give, cols)
        residual = excitation - current - summed
        current = current + damping * residual
    return (current, residual)


def solution(mesh):
    in_specs = (
        P("row", "col"),
        P(("row", "col"), None),
        P(("row", "col"), None, None),
        P(("row", "col"), None, None),
        P(("row", "col"), None),
    )
    out_specs = (P(("row", "col"), None), P(("row", "col"), None))
    return jax.shard_map(steps, mesh=mesh, in_specs=in_specs, out_specs=out_specs, check_vma=False)
```

```python
import functools

import jax
import jax.numpy as jnp
from jax import lax
from jax.experimental import pallas as pl
from jax.experimental.pallas import tpu as pltpu
from jax.sharding import PartitionSpec as P


ITERS = 2
NADJ = 6

damping = 0.25
face_weight = 0.25

BF = jnp.bfloat16
F32 = jnp.float32

PARAMS = pltpu.CompilerParams(vmem_limit_bytes=16 * 2**20)


def dot(a, b):
    return jnp.dot(a, b, preferred_element_type=F32)


def dot_t(a, b):
    return lax.dot_general(a, b, (((0,), (0,)), ((), ())), preferred_element_type=F32)


def exchange(blocks, axis):
    return lax.all_to_all(blocks, axis, split_axis=0, concat_axis=0, tiled=True)


def turned(rows, cols):
    per_col = rows // cols
    return [
        (r * cols + c, ((r % per_col) * cols + c) * cols + r // per_col)
        for r in range(rows)
        for c in range(cols)
    ]


def rotated(col, k, peers):
    return (col + k) & (peers - 1)


def owner(col, distance, j, peers):
    return rotated(col, -2 * distance, peers) ^ j


def assemble_kernel(outs, col_ref, *refs):
    pair_refs, group_ref = refs[:-outs], refs[-outs]
    peers = 2 * len(pair_refs)
    n = group_ref.shape[0] // peers
    for d, pair_ref in enumerate(pair_refs):
        for j in range(2):
            s = owner(col_ref[0], d, j, peers)
            group_ref[pl.ds(pl.multiple_of(s * n, n), n), :] = pair_ref[j, :n, :]
            if outs == 2:
                refs[-1][s] = pair_ref[j, n:, :].astype(F32)


def volume_kernel(interp_ref, dtn_ref, group_ref, *refs):
    traces = dot(interp_ref[...], group_ref[...]).astype(BF)
    response = dot(dtn_ref[...], traces).astype(BF)
    total = dot_t(interp_ref[...], response)
    if len(refs) == 2:
        total = total + refs[0][...]
    refs[-1][...] = total


def faces_kernel(has_prior, col_ref, mix_ref, group_ref, *refs):
    peers = mix_ref.shape[0]
    slice_refs, prior_refs = refs[:peers], refs[peers : peers + has_prior]
    out_refs, traces_ref = refs[peers + has_prior : -1], refs[-1]
    group = group_ref[...]
    for k in range(peers):
        traces_ref[rotated(col_ref[0], -k, peers)] = dot(slice_refs[k][...], group)
    total = prior_refs[0][...] if prior_refs else None
    for k in range(peers):
        row = mix_ref[rotated(col_ref[0], -k, peers)][:1]
        mixed = None
        for p in range(peers):
            term = row[:, p : p + 1] * traces_ref[p]
            mixed = term if mixed is None else mixed + term
        term = dot_t(slice_refs[k][...], mixed.astype(BF))
        total = term if total is None else total + term
    if len(out_refs) == 1:
        out_refs[0][...] = total
    else:
        divide(col_ref[0], total, traces_ref, *out_refs)


def divide(col, total, blocks_ref, keep_ref, give_ref):
    peers, n, ne = blocks_ref.shape
    blocks_ref[...] = total.reshape(peers, n, ne)
    for d in range(peers // 2):
        keep_ref[d] = blocks_ref[col ^ (2 * d)]
        give_ref[d] = blocks_ref[col ^ (2 * d + 1)].astype(BF)


def surface_kernel(col_ref, prior_ref, surface_ref, column_ref, *refs):
    total = prior_ref[...] + dot(surface_ref[...], column_ref[...])
    if len(refs) == 1:
        refs[0][...] = total
    else:
        divide(col_ref[0], total, refs[2], *refs[:2])


def divided(peers, shape):
    n, ne = shape[0] // peers, shape[1]
    return [
        jax.ShapeDtypeStruct((peers // 2, n, ne), F32),
        jax.ShapeDtypeStruct((peers // 2, n, ne), BF),
    ]


def repeated_kernel(piece_ref, out_ref, sems):
    copies = [
        pltpu.make_async_copy(piece_ref, out_ref.at[i], sems.at[i]) for i in range(out_ref.shape[0])
    ]
    for copy in copies:
        copy.start()
    for copy in copies:
        copy.wait()


def repeated(piece, count):
    return pl.pallas_call(
        repeated_kernel,
        out_shape=jax.ShapeDtypeStruct((count, *piece.shape), piece.dtype),
        in_specs=[vmem()],
        out_specs=pl.BlockSpec(memory_space=pl.ANY),
        scratch_shapes=[pltpu.SemaphoreType.DMA((count,))],
        compiler_params=PARAMS,
        name="repeated",
    )(piece)


def vmem():
    return pl.BlockSpec(memory_space=pltpu.VMEM)


def cost(products, m, k, ne):
    return pl.CostEstimate(
        flops=2 * products * m * k * ne, bytes_accessed=2 * products * m * k, transcendentals=0
    )


def smem():
    return pl.BlockSpec(memory_space=pltpu.SMEM)


def assemble(place, pairs, n):
    peers, (_, high, ne) = 2 * len(pairs), pairs[0].shape
    shapes = [jax.ShapeDtypeStruct((peers * n, ne), BF)]
    if high > n:
        shapes.append(jax.ShapeDtypeStruct((peers, high - n, ne), F32))
    return pl.pallas_call(
        functools.partial(assemble_kernel, len(shapes)),
        out_shape=shapes,
        in_specs=[smem()] + [vmem()] * len(pairs),
        out_specs=[vmem()] * len(shapes),
        compiler_params=PARAMS,
        name="assemble",
    )(place, *pairs)


def volume(interp, dtn, group, *prior):
    m, rb = interp.shape
    ne = group.shape[-1]
    return pl.pallas_call(
        volume_kernel,
        out_shape=jax.ShapeDtypeStruct((rb, ne), F32),
        in_specs=[vmem()] * (3 + len(prior)),
        out_specs=vmem(),
        compiler_params=PARAMS,
        cost_estimate=cost(3, m, rb, ne),
        name="volume",
    )(interp, dtn, group, *prior)


def applied(place, prior, surface, column_block, peers=0):
    (m, k), ne = surface.shape, prior.shape[1]
    plain = [jax.ShapeDtypeStruct(prior.shape, F32)]
    shapes = divided(peers, prior.shape) if peers else plain
    return pl.pallas_call(
        surface_kernel,
        out_shape=shapes,
        in_specs=[smem()] + [vmem()] * 3,
        out_specs=[vmem()] * len(shapes),
        scratch_shapes=[pltpu.VMEM((peers, m // peers, ne), F32)] if peers else [],
        compiler_params=PARAMS,
        cost_estimate=cost(1, m, k, ne),
        name="applied",
    )(place, prior, surface, column_block)


def faces(place, mix, group, slices, *prior):
    (ms, rb), ne = slices[0].shape, group.shape[-1]
    peers = len(slices)
    plain = [jax.ShapeDtypeStruct((rb, ne), F32)]
    shapes = divided(peers, (rb, ne)) if prior else plain
    return pl.pallas_call(
        functools.partial(faces_kernel, len(prior)),
        out_shape=shapes,
        in_specs=[smem()] + [vmem()] * (2 + peers + len(prior)),
        out_specs=[vmem()] * len(shapes),
        scratch_shapes=[pltpu.VMEM((peers, ms, ne), F32)],
        compiler_params=PARAMS,
        cost_estimate=cost(2, peers * ms, rb, ne),
        name="faces",
    )(place, mix, group, *slices, *prior)


def swapped(shard, cols, bits=1):
    return lax.ppermute(shard, "col", [(i, i ^ bits) for i in range(cols)])


def along(shard, d, cols):
    return lax.ppermute(shard, "col", [(i, (i + 2 * d) % cols) for i in range(cols)])


def summed_over(keep, give, cols):
    taken = swapped(give, cols)
    sums = keep + taken.astype(F32)
    taken = swapped(sums[1:3].astype(BF), cols, 2).astype(F32)
    last = swapped((sums[3] + taken[1]).astype(BF), cols, 6).astype(F32)
    return sums[0] + taken[0] + last


def gathered(shard, cols):
    other = swapped(shard, cols)
    pair = jnp.stack([shard, other])
    pairs = [pair]
    for d in range(1, cols // 2):
        pairs.append(along(pair, d, cols))
    return pairs


def steps(surface, excitation, dtn_blocks, interp_blocks, adjacency):
    cols = lax.axis_size("col")
    rows = lax.axis_size("row")
    col = lax.axis_index("col")
    place = col.astype(jnp.int32)[None]
    dtn = dtn_blocks[0]
    interp = interp_blocks[0]
    ms = interp.shape[0] // cols
    n, ne = excitation.shape

    slices = []
    for k in range(cols):
        block = lax.dynamic_slice_in_dim(interp, rotated(col, k, cols) * ms, ms, 0)
        if k:
            block = lax.ppermute(block, "col", [(i, (i + k) % cols) for i in range(cols)])
        slices.append(block)

    adjacent = adjacency[0] & (cols - 1)
    owners = jnp.arange(ne, dtype=jnp.int32)
    counts = jnp.sum((adjacent[None, :] == owners[:, None]).astype(F32), axis=1)
    me = (owners == col).astype(F32)
    weights = (1.0 + face_weight * NADJ) * me - face_weight * counts
    extra = jnp.broadcast_to(weights.astype(BF)[None, :], (16, ne))

    current = excitation
    residual = excitation
    mix = None
    for sweep in range(ITERS):
        rounded = current.astype(BF)
        piece = lax.ppermute(rounded, ("row", "col"), turned(rows, cols))
        column_block = exchange(repeated(piece, rows), "row").reshape(rows * n, ne)
        sent = jnp.concatenate([rounded, extra], axis=0) if sweep == 0 else rounded
        pairs = gathered(sent, cols)
        group, *rows_got = assemble(place, pairs, n)
        if sweep == 0:
            mix = rows_got[0]
            own = volume(interp, dtn, group)
            wide = applied(place, own, surface, column_block)[0]
            keep, give = faces(place, mix, group, slices, wide)
        else:
            wide = faces(place, mix, group, slices)[0]
            own = volume(interp, dtn, group, wide)
            keep, give = applied(place, own, surface, column_block, cols)
        summed = summed_over(keep, give, cols)
        residual = excitation - current - summed
        current = current + damping * residual
    return (current, residual)


def solution(mesh):
    in_specs = (
        P("row", "col"),
        P(("row", "col"), None),
        P(("row", "col"), None, None),
        P(("row", "col"), None, None),
        P(("row", "col"), None),
    )
    out_specs = (P(("row", "col"), None), P(("row", "col"), None))
    return jax.shard_map(steps, mesh=mesh, in_specs=in_specs, out_specs=out_specs, check_vma=False)
```

```python
import functools

import jax
import jax.numpy as jnp
from jax import lax
from jax.experimental import pallas as pl
from jax.experimental.pallas import tpu as pltpu
from jax.sharding import PartitionSpec as P


ITERS = 2
NADJ = 6

damping = 0.25
face_weight = 0.25

BF = jnp.bfloat16
F32 = jnp.float32

PARAMS = pltpu.CompilerParams(vmem_limit_bytes=16 * 2**20)


def dot(a, b):
    return jnp.dot(a, b, preferred_element_type=F32)


def dot_t(a, b):
    return lax.dot_general(a, b, (((0,), (0,)), ((), ())), preferred_element_type=F32)


def exchange(blocks, axis):
    return lax.all_to_all(blocks, axis, split_axis=0, concat_axis=0, tiled=True)


def copy_for_each(shard, axis):
    return exchange(jnp.broadcast_to(shard, (lax.axis_size(axis), *shard.shape)), axis)


def turned(rows, cols):
    per_col = rows // cols
    return [
        (r * cols + c, ((r % per_col) * cols + c) * cols + r // per_col)
        for r in range(rows)
        for c in range(cols)
    ]


def rotated(col, k, peers):
    return (col + k) & (peers - 1)


def owner(col, distance, j, peers):
    return rotated(col, -2 * distance, peers) ^ j


def assemble_kernel(outs, col_ref, *refs):
    pair_refs, group_ref = refs[:-outs], refs[-outs]
    peers = 2 * len(pair_refs)
    n = group_ref.shape[0] // peers
    for d, pair_ref in enumerate(pair_refs):
        for j in range(2):
            s = owner(col_ref[0], d, j, peers)
            group_ref[pl.ds(pl.multiple_of(s * n, n), n), :] = pair_ref[j, :n, :]
            if outs == 2:
                refs[-1][s] = pair_ref[j, n:, :].astype(F32)


def volume_kernel(interp_ref, dtn_ref, group_ref, *refs):
    traces = dot(interp_ref[...], group_ref[...]).astype(BF)
    response = dot(dtn_ref[...], traces).astype(BF)
    total = dot_t(interp_ref[...], response)
    if len(refs) == 2:
        total = total + refs[0][...]
    refs[-1][...] = total


def faces_kernel(has_prior, col_ref, mix_ref, group_ref, *refs):
    peers = mix_ref.shape[0]
    slice_refs, prior_refs = refs[:peers], refs[peers : peers + has_prior]
    out_refs, traces_ref = refs[peers + has_prior : -1], refs[-1]
    group = group_ref[...]
    for k in range(peers):
        traces_ref[rotated(col_ref[0], -k, peers)] = dot(slice_refs[k][...], group)
    total = prior_refs[0][...] if prior_refs else None
    for k in range(peers):
        row = mix_ref[rotated(col_ref[0], -k, peers)][:1]
        mixed = None
        for p in range(peers):
            term = row[:, p : p + 1] * traces_ref[p]
            mixed = term if mixed is None else mixed + term
        term = dot_t(slice_refs[k][...], mixed.astype(BF))
        total = term if total is None else total + term
    if len(out_refs) == 1:
        out_refs[0][...] = total
    else:
        divide(col_ref[0], total, traces_ref, *out_refs)


def divide(col, total, blocks_ref, keep_ref, give_ref):
    peers, n, ne = blocks_ref.shape
    blocks_ref[...] = total.reshape(peers, n, ne)
    for d in range(peers // 2):
        keep_ref[d] = blocks_ref[rotated(col, 2 * d, peers)]
        give_ref[d] = blocks_ref[rotated(col, 2 * d, peers) ^ 1].astype(BF)


def surface_kernel(col_ref, prior_ref, surface_ref, column_ref, *refs):
    total = prior_ref[...] + dot(surface_ref[...], column_ref[...])
    if len(refs) == 1:
        refs[0][...] = total
    else:
        divide(col_ref[0], total, refs[2], *refs[:2])


def divided(peers, shape):
    n, ne = shape[0] // peers, shape[1]
    return [
        jax.ShapeDtypeStruct((peers // 2, n, ne), F32),
        jax.ShapeDtypeStruct((peers // 2, n, ne), BF),
    ]


def vmem():
    return pl.BlockSpec(memory_space=pltpu.VMEM)


def cost(products, m, k, ne):
    return pl.CostEstimate(
        flops=2 * products * m * k * ne, bytes_accessed=2 * products * m * k, transcendentals=0
    )


def smem():
    return pl.BlockSpec(memory_space=pltpu.SMEM)


def assemble(place, pairs, n):
    peers, (_, high, ne) = 2 * len(pairs), pairs[0].shape
    shapes = [jax.ShapeDtypeStruct((peers * n, ne), BF)]
    if high > n:
        shapes.append(jax.ShapeDtypeStruct((peers, high - n, ne), F32))
    return pl.pallas_call(
        functools.partial(assemble_kernel, len(shapes)),
        out_shape=shapes,
        in_specs=[smem()] + [vmem()] * len(pairs),
        out_specs=[vmem()] * len(shapes),
        compiler_params=PARAMS,
        name="assemble",
    )(place, *pairs)


def volume(interp, dtn, group, *prior):
    m, rb = interp.shape
    ne = group.shape[-1]
    return pl.pallas_call(
        volume_kernel,
        out_shape=jax.ShapeDtypeStruct((rb, ne), F32),
        in_specs=[vmem()] * (3 + len(prior)),
        out_specs=vmem(),
        compiler_params=PARAMS,
        cost_estimate=cost(3, m, rb, ne),
        name="volume",
    )(interp, dtn, group, *prior)


def traces_kernel(interp_ref, group_ref, out_ref):
    out_ref[...] = dot(interp_ref[...], group_ref[...]).astype(BF)


def response_kernel(interp_ref, dtn_ref, traces_ref, out_ref):
    response = dot(dtn_ref[...], traces_ref[...]).astype(BF)
    out_ref[...] = dot_t(interp_ref[...], response)


def volume_in_two(interp, dtn, group):
    m, rb = interp.shape
    ne = group.shape[-1]
    traces = pl.pallas_call(
        traces_kernel,
        out_shape=jax.ShapeDtypeStruct((m, ne), BF),
        in_specs=[vmem()] * 2,
        out_specs=vmem(),
        compiler_params=PARAMS,
        cost_estimate=cost(1, m, rb, ne),
        name="traces",
    )(interp, group)
    return pl.pallas_call(
        response_kernel,
        out_shape=jax.ShapeDtypeStruct((rb, ne), F32),
        in_specs=[vmem()] * 3,
        out_specs=vmem(),
        compiler_params=PARAMS,
        cost_estimate=cost(2, m, rb, ne),
        name="response",
    )(interp, dtn, traces)


def applied(place, prior, surface, column_block, peers=0):
    (m, k), ne = surface.shape, prior.shape[1]
    plain = [jax.ShapeDtypeStruct(prior.shape, F32)]
    shapes = divided(peers, prior.shape) if peers else plain
    return pl.pallas_call(
        surface_kernel,
        out_shape=shapes,
        in_specs=[smem()] + [vmem()] * 3,
        out_specs=[vmem()] * len(shapes),
        scratch_shapes=[pltpu.VMEM((peers, m // peers, ne), F32)] if peers else [],
        compiler_params=PARAMS,
        cost_estimate=cost(1, m, k, ne),
        name="applied",
    )(place, prior, surface, column_block)


def faces(place, mix, group, slices, *prior):
    (ms, rb), ne = slices[0].shape, group.shape[-1]
    peers = len(slices)
    plain = [jax.ShapeDtypeStruct((rb, ne), F32)]
    shapes = divided(peers, (rb, ne)) if prior else plain
    return pl.pallas_call(
        functools.partial(faces_kernel, len(prior)),
        out_shape=shapes,
        in_specs=[smem()] + [vmem()] * (2 + peers + len(prior)),
        out_specs=[vmem()] * len(shapes),
        scratch_shapes=[pltpu.VMEM((peers, ms, ne), F32)],
        compiler_params=PARAMS,
        cost_estimate=cost(2, peers * ms, rb, ne),
        name="faces",
    )(place, mix, group, *slices, *prior)


def swapped(shard, cols):
    return lax.ppermute(shard, "col", [(i, i ^ 1) for i in range(cols)])


def along(shard, d, cols):
    return lax.ppermute(shard, "col", [(i, (i + 2 * d) % cols) for i in range(cols)])


def summed_over(keep, give, cols):
    taken = swapped(give, cols)
    sums = keep + taken.astype(F32)
    total = sums[0]
    for d in range(1, cols // 2):
        total = total + along(sums[d].astype(BF), d, cols).astype(F32)
    return total


def gathered(shard, cols):
    other = swapped(shard, cols)
    pair = jnp.stack([shard, other])
    pairs = [pair]
    for d in range(1, cols // 2):
        pairs.append(along(pair, d, cols))
    return pairs


def steps(surface, excitation, dtn_blocks, interp_blocks, adjacency):
    cols = lax.axis_size("col")
    rows = lax.axis_size("row")
    col = lax.axis_index("col")
    place = col.astype(jnp.int32)[None]
    dtn = dtn_blocks[0]
    interp = interp_blocks[0]
    ms = interp.shape[0] // cols
    n, ne = excitation.shape

    slices = []
    for k in range(cols):
        block = lax.dynamic_slice_in_dim(interp, rotated(col, k, cols) * ms, ms, 0)
        if k:
            block = lax.ppermute(block, "col", [(i, (i + k) % cols) for i in range(cols)])
        slices.append(block)

    adjacent = adjacency[0] & (cols - 1)
    owners = jnp.arange(ne, dtype=jnp.int32)
    counts = jnp.sum((adjacent[None, :] == owners[:, None]).astype(F32), axis=1)
    me = (owners == col).astype(F32)
    weights = (1.0 + face_weight * NADJ) * me - face_weight * counts
    extra = jnp.broadcast_to(weights.astype(BF)[None, :], (16, ne))

    current = excitation
    residual = excitation
    mix = None
    for sweep in range(ITERS):
        rounded = current.astype(BF)
        piece = lax.ppermute(rounded, ("row", "col"), turned(rows, cols))
        column_block = copy_for_each(piece, "row").reshape(rows * n, ne)
        sent = jnp.concatenate([rounded, extra], axis=0) if sweep == 0 else rounded
        pairs = gathered(sent, cols)
        group, *rows_got = assemble(place, pairs, n)
        if sweep == 0:
            mix = rows_got[0]
            own = volume_in_two(interp, dtn, group)
            wide = applied(place, own, surface, column_block)[0]
            keep, give = faces(place, mix, group, slices, wide)
        else:
            wide = faces(place, mix, group, slices)[0]
            own = volume(interp, dtn, group, wide)
            keep, give = applied(place, own, surface, column_block, cols)
        summed = summed_over(keep, give, cols)
        residual = excitation - current - summed
        current = current + damping * residual
    return (current, residual)


def solution(mesh):
    in_specs = (
        P("row", "col"),
        P(("row", "col"), None),
        P(("row", "col"), None, None),
        P(("row", "col"), None, None),
        P(("row", "col"), None),
    )
    out_specs = (P(("row", "col"), None), P(("row", "col"), None))
    return jax.shard_map(steps, mesh=mesh, in_specs=in_specs, out_specs=out_specs, check_vma=False)
```
